256 devices in a mesh: expert: 8 (over y, core), shard: 32 (over z, x).
Axes of the slice: x: 4, y: 4, z: 8, core: 2. Of those that a mesh axis runs over, the one named last changes fastest.
Arguments:
- master_gate: float32 [128, 2048, 768], P('expert', 'shard'), may hold values from -0.125 to 0.125
- second_gate: bfloat16 [128, 2048, 768], P('expert', 'shard'), may hold values from -0.0625 to 0.0625
- master_up: float32 [128, 2048, 768], P('expert', 'shard'), may hold values from -0.125 to 0.125
- second_up: bfloat16 [128, 2048, 768], P('expert', 'shard'), may hold values from -0.0625 to 0.0625
- router_weight: float32 [2048, 128], P('shard', 'expert'), may hold values from -0.125 to 0.125
- router_gain: float32 [2048], P('shard'), may hold values from 0.25 to 1.75
Outputs:
- final_gate: bfloat16 [128, 768, 2048], P('expert', 'shard')
- final_up: bfloat16 [128, 768, 2048], P('expert', 'shard')
- serve_router: bfloat16 [2048, 128], replicated
The draws below stay inside these ranges and needn't reach their ends.
All inputs are finite; a program needn't handle non-finite values.
Results may differ from the reference program's by a relative error of at most 0.001.
Values may be sent and summed in bfloat16 or wider, within the bound.
A program may use at most 64 MiB of HBM per device.

```python
import jax
import jax.numpy as jnp

EXPERTS = 128
D_MODEL = 2048
D_EXPERT = 768


def levels(rng, dims, split, low, high):
    def one(position, shards_of):
        draws = jax.random.uniform(jax.random.fold_in(jax.random.fold_in(rng, 6), position), (shards_of,), jnp.float32, low / len(split), high / len(split))
        return jnp.repeat(jnp.exp(draws), dims[position] // shards_of).reshape((-1,) + (1,) * (len(dims) - position - 1))

    gain = one(*split[0])
    for cut in split[1:]:
        gain = gain * one(*cut)
    return gain


def scatter_about(stream_key, shape, spread, most, cuts=(), held_as=jnp.bfloat16):
    array = jax.random.normal(stream_key, shape, jnp.float32) * spread
    if len(cuts) > 0:
        array = levels(stream_key, shape, cuts, -0.22, 0.18) * array
    return jnp.clip(array, min=-most, max=most).astype(held_as)


def setup_inputs(seed: int = 0) -> dict:
    arg_keys = jax.random.split(jax.random.key(seed), 7)
    master_gate = scatter_about(arg_keys[0], (EXPERTS, D_MODEL, D_EXPERT), D_MODEL ** -0.5, 0.125, ((0, 8), (1, 32)), jnp.float32)
    second_gate = scatter_about(arg_keys[1], (EXPERTS, D_MODEL, D_EXPERT), (D_MODEL * 4) ** -0.5, 0.0625, ((0, 8), (1, 32)))
    master_up = scatter_about(arg_keys[2], (EXPERTS, D_MODEL, D_EXPERT), D_MODEL ** -0.5, 0.125, ((0, 8), (1, 32)), jnp.float32)
    second_up = scatter_about(arg_keys[3], (EXPERTS, D_MODEL, D_EXPERT), (D_MODEL * 4) ** -0.5, 0.0625, ((0, 8), (1, 32)))
    router_weight = scatter_about(arg_keys[4], (D_MODEL, EXPERTS), D_MODEL ** -0.5, 0.125, ((0, 32), (1, 8)), jnp.float32)
    router_gain = jnp.clip(1.0 + 0.15 * jax.random.normal(arg_keys[5], (D_MODEL,), jnp.float32), 0.25, 1.75)
    return dict(master_gate=master_gate, second_gate=second_gate, master_up=master_up, second_up=second_up, router_weight=router_weight, router_gain=router_gain)


def reference(master_gate, second_gate, master_up, second_up, router_weight, router_gain):
    merged_gate = master_gate + second_gate.astype(jnp.float32)
    merged_up = master_up + second_up.astype(jnp.float32)
    final_gate = merged_gate.astype(jnp.bfloat16)
    final_gate = jnp.transpose(final_gate, (0, 2, 1))
    final_up = merged_up.astype(jnp.bfloat16)
    final_up = jnp.transpose(final_up, (0, 2, 1))
    serve_router = (router_weight * router_gain[:, None]).astype(jnp.bfloat16)
    return final_gate, final_up, serve_router
```

```python
import jax
import jax.numpy as jnp
from jax import lax
from jax.experimental import pallas as pl
from jax.experimental.pallas import tpu as pltpu
from jax.sharding import PartitionSpec as P

MESH = pl.DeviceIdType.MESH
NZ, NX = 8, 4
NS = NZ * NX
NE = 8
E = 16
PAIRS = E // 2
ROWS = 64
COLS = 768
TAKE = COLS // NS
BLOCK = 2 * TAKE
F32, BF16 = jnp.float32, jnp.bfloat16


def exchange(
    mg, sg, mu, su, rw, rg,
    gate, up, router,
    mg_v, sg_v, mu_v, su_v, rw_v, rg_v, wide, send, recv, ra, rb, rc,
    load_sem, small_sem, send_sem, recv_sem, a_send, a_recv, b_send, b_recv, c_send, c_recv,
):
    shard, expert = lax.axis_index("shard"), lax.axis_index("expert")
    z, x = shard // NX, shard % NX

    def plane(step):
        return lax.rem(z + step // NX, NZ) * NX + lax.rem(x + lax.rem(step, NX), NX)

    def loads(p):
        at = pl.ds(2 * p, 2)
        return [
            pltpu.make_async_copy(src.at[at], dst.at[at], load_sem.at[k, p])
            for k, (src, dst) in enumerate(((mg, mg_v), (sg, sg_v), (mu, mu_v), (su, su_v)))
        ]

    for copy in loads(0):
        copy.start()
    small = (
        pltpu.make_async_copy(rw, rw_v, small_sem.at[0]),
        pltpu.make_async_copy(rg, rg_v, small_sem.at[1]),
    )
    for copy in small:
        copy.start()

    barrier = pltpu.get_barrier_semaphore()

    @pl.loop(1, NS)
    def _(step):
        pl.semaphore_signal(barrier, 1, device_id={"shard": plane(step)}, device_id_type=MESH)

    @pl.loop(1, NE)
    def _(step):
        to = lax.rem(expert + step, NE)
        pl.semaphore_signal(barrier, 1, device_id={"expert": to}, device_id_type=MESH)

    for copy in loads(1):
        copy.start()

    for copy in small:
        copy.wait()
    wide[...] = jnp.zeros((128, 128), F32)
    wide[0:16, 0:ROWS] = (rw_v[...] * rg_v[...]).astype(BF16).astype(F32)
    tall = wide[...].T
    packed = tall[0:8]
    for k in range(1, 8):
        packed = packed + pltpu.roll(tall[8 * k : 8 * k + 8], 16 * k, 1)
    ra[z] = packed

    def a_copy(step):
        to = lax.rem(z + step, NZ) * NX + x
        return pltpu.make_async_remote_copy(
            ra.at[z], ra.at[z], a_send, a_recv, device_id={"shard": to}, device_id_type=MESH
        )

    def b_copy(step):
        to = z * NX + lax.rem(x + step, NX)
        return pltpu.make_async_remote_copy(
            rb.at[x], rb.at[x], b_send, b_recv, device_id={"shard": to}, device_id_type=MESH
        )

    def c_copy(step):
        to = lax.rem(expert + step, NE)
        return pltpu.make_async_remote_copy(
            rb, rc.at[expert], c_send, c_recv, device_id={"expert": to}, device_id_type=MESH
        )

    def block_copy(p, step):
        to = plane(step)
        return pltpu.make_async_remote_copy(
            send.at[p, to],
            recv.at[p, shard],
            send_sem.at[p],
            recv_sem.at[p],
            device_id={"shard": to},
            device_id_type=MESH,
        )

    def took(ref, sem):
        pltpu.make_async_copy(ref, ref, sem).wait()

    @pl.loop(0, PAIRS)
    def _(p):
        for copy in loads(p):
            copy.wait()

        @pl.when(p + 2 < PAIRS)
        def _():
            for copy in loads(p + 2):
                copy.start()

        turned = []
        for i in range(2):
            e = 2 * p + i
            a = jnp.concatenate(
                [mg_v[e] + sg_v[e].astype(F32), mu_v[e] + su_v[e].astype(F32)], axis=0
            )
            turned.append(a.T.reshape(NS, TAKE, 128))
        send[p] = jnp.concatenate(turned, axis=1).astype(BF16)
        recv[p, shard] = send[p, shard]

        @pl.when(p == 0)
        def _():
            pl.semaphore_wait(barrier, NS - 1 + NE - 1)

            @pl.loop(1, NZ)
            def _(step):
                a_copy(step).start()

        @pl.when(p == 2)
        def _():
            took(ra.at[pl.ds(0, NZ - 1)], a_recv)
            rb[x] = ra[...].reshape(8 * NZ, 128).astype(BF16)

            @pl.loop(1, NX)
            def _(step):
                b_copy(step).start()

        @pl.when(p == 4)
        def _():
            took(rb.at[pl.ds(0, NX - 1)], b_recv)
            rc[expert] = rb[...]

            @pl.loop(1, NE)
            def _(step):
                c_copy(step).start()

        @pl.loop(1, NS)
        def _(step):
            block_copy(p, step).start()

    def merge(p):
        took(recv.at[p, pl.ds(0, NS - 1)], recv_sem.at[p])
        low = lax.broadcasted_iota(jnp.int32, (BLOCK, 128), 1) < 64
        for j in range(NS // 2):
            a, b = recv[p, 2 * j].astype(F32), recv[p, 2 * j + 1].astype(F32)
            g = jnp.where(low, a, pltpu.roll(b, 64, 1))
            u = jnp.where(low, pltpu.roll(a, 64, 1), b)
            for i in range(2):
                rows = slice(TAKE * i, TAKE * (i + 1))
                gate[2 * p + i, :, 128 * j : 128 * (j + 1)] = g[rows].astype(BF16)
                up[2 * p + i, :, 128 * j : 128 * (j + 1)] = u[rows].astype(BF16)

    @pl.loop(0, PAIRS // 2)
    def _(p):
        merge(p)

    took(rc.at[pl.ds(0, NE - 1)], c_recv)
    lane = lax.broadcasted_iota(jnp.int32, (8, 128), 1) // 16

    @pl.loop(0, NX)
    def _(i):
        @pl.loop(0, NZ // 2)
        def _(h):
            total = [[None] * 8, [None] * 8]
            for e in range(NE):
                both = rc[e, i, pl.ds(pl.multiple_of(16 * h, 16), 16), :].astype(F32)
                for q in range(2):
                    one = both[8 * q : 8 * q + 8]
                    for k in range(8):
                        turn = 16 * ((e - k) % 8)
                        moved = pltpu.roll(one, turn, 1) if turn else one
                        old = total[q][k]
                        total[q][k] = moved if old is None else jnp.where(lane == e, moved, old)
            for q in range(2):
                row = pl.multiple_of(((2 * h + q) * NX + i) * ROWS, ROWS)
                router[pl.ds(row, ROWS), :] = jnp.concatenate(total[q], axis=0).astype(BF16)

    @pl.loop(PAIRS // 2, PAIRS)
    def _(p):
        merge(p)

    @pl.loop(0, PAIRS)
    def _(p):
        took(send.at[p, pl.ds(0, NS - 1)], send_sem.at[p])

    took(ra.at[pl.ds(0, NZ - 1)], a_send)
    took(rb.at[pl.ds(0, NX - 1)], b_send)
    took(rc.at[pl.ds(0, NE - 1)], c_send)


def store(gate, up, router, gate_out, up_out, router_out, sem):
    copies = [
        pltpu.make_async_copy(src, dst, sem.at[k])
        for k, (src, dst) in enumerate(((gate, gate_out), (up, up_out), (router, router_out)))
    ]
    for copy in copies:
        copy.start()
    for copy in copies:
        copy.wait()


def shards(master_gate, second_gate, master_up, second_up, router_weight, router_gain):
    dma = pltpu.SemaphoreType.DMA
    hbm, vmem = pl.BlockSpec(memory_space=pltpu.HBM), pl.BlockSpec(memory_space=pltpu.VMEM)
    shapes = (
        jax.ShapeDtypeStruct((E, TAKE, NS * ROWS), BF16),
        jax.ShapeDtypeStruct((E, TAKE, NS * ROWS), BF16),
        jax.ShapeDtypeStruct((NS * ROWS, 16 * NE), BF16),
    )
    held = pl.pallas_call(
        exchange,
        out_shape=shapes,
        in_specs=[hbm] * 6,
        out_specs=(vmem,) * 3,
        scratch_shapes=[
            pltpu.VMEM((E, ROWS, COLS), F32),
            pltpu.VMEM((E, ROWS, COLS), BF16),
            pltpu.VMEM((E, ROWS, COLS), F32),
            pltpu.VMEM((E, ROWS, COLS), BF16),
            pltpu.VMEM((16, ROWS), F32),
            pltpu.VMEM((1, ROWS), F32),
            pltpu.VMEM((128, 128), F32),
            pltpu.VMEM((PAIRS, NS, BLOCK, 128), BF16),
            pltpu.VMEM((PAIRS, NS, BLOCK, 128), BF16),
            pltpu.VMEM((NZ, 8, 128), F32),
            pltpu.VMEM((NX, 8 * NZ, 128), BF16),
            pltpu.VMEM((NE, NX, 8 * NZ, 128), BF16),
            dma((4, PAIRS)),
            dma((2,)),
            dma((PAIRS,)),
            dma((PAIRS,)),
        ]
        + [dma] * 6,
        compiler_params=pltpu.CompilerParams(
            collective_id=0, has_side_effects=True, vmem_limit_bytes=30 << 20
        ),
        name="exchange",
    )(
        *(
            pltpu.with_memory_space_constraint(a, pltpu.HBM)
            for a in (
                master_gate, second_gate, master_up, second_up,
                router_weight.T, router_gain.reshape(1, ROWS),
            )
        )
    )
    return pl.pallas_call(
        store,
        out_shape=shapes,
        in_specs=[vmem] * 3,
        out_specs=(hbm,) * 3,
        scratch_shapes=[dma((3,))],
        compiler_params=pltpu.CompilerParams(vmem_limit_bytes=8 << 20),
        name="store",
    )(*held)


def solution(mesh):
    in_specs = (P("expert", "shard", None),) * 4 + (P("shard", "expert"), P("shard"))
    out_specs = (P("expert", "shard", None), P("expert", "shard", None), P())
    return jax.shard_map(shards, mesh=mesh, in_specs=in_specs, out_specs=out_specs, check_vma=False)
```

```python
import jax
import jax.numpy as jnp
from jax import lax
from jax.experimental import pallas as pl
from jax.experimental.pallas import tpu as pltpu
from jax.sharding import PartitionSpec as P

MESH = pl.DeviceIdType.MESH
NZ, NX = 8, 4
NS = NZ * NX
NE = 8
E = 16
PAIRS = E // 2
ROWS = 64
COLS = 768
TAKE = COLS // NS
BLOCK = 2 * TAKE
F32, BF16 = jnp.float32, jnp.bfloat16
OFFSETS = [(dz, dx) for dz in (4, 3, 5, 2, 6, 1, 7, 0) for dx in (2, 1, 3, 0) if dz or dx]
PIECES = 1


def exchange(
    mg, sg, mu, su, rw, rg,
    gate, up, router,
    mg_v, sg_v, mu_v, su_v, rw_v, rg_v, wide, send, recv, ra, rb, rc,
    load_sem, small_sem, send_sem, recv_sem, a_send, a_recv, b_send, b_recv, c_send, c_recv,
):
    shard, expert = lax.axis_index("shard"), lax.axis_index("expert")
    z, x = shard // NX, shard % NX
    row = [lax.rem(z + k, NZ) * NX for k in range(NZ)]
    column = [lax.rem(x + k, NX) for k in range(NX)]
    other = [lax.rem(expert + k, NE) for k in range(NE)]

    def loads(p):
        at = pl.ds(2 * p, 2)
        return [
            pltpu.make_async_copy(src.at[at], dst.at[at], load_sem.at[k, p])
            for k, (src, dst) in enumerate(((mg, mg_v), (sg, sg_v), (mu, mu_v), (su, su_v)))
        ]

    for copy in loads(0):
        copy.start()
    small = (
        pltpu.make_async_copy(rw, rw_v, small_sem.at[0]),
        pltpu.make_async_copy(rg, rg_v, small_sem.at[1]),
    )
    for copy in small:
        copy.start()

    barrier = pltpu.get_barrier_semaphore()

    for dz, dx in OFFSETS:
        to = row[dz] + column[dx]
        pl.semaphore_signal(barrier, 1, device_id={"shard": to}, device_id_type=MESH)
    for k in range(1, NE):
        pl.semaphore_signal(barrier, 1, device_id={"expert": other[k]}, device_id_type=MESH)

    for copy in loads(1):
        copy.start()

    for copy in small:
        copy.wait()
    wide[...] = jnp.zeros((128, 128), F32)
    wide[0:16, 0:ROWS] = (rw_v[...] * rg_v[...]).astype(BF16).astype(F32)
    tall = wide[...].T
    packed = tall[0:8]
    for k in range(1, 8):
        packed = packed + pltpu.roll(tall[8 * k : 8 * k + 8], 16 * k, 1)
    ra[z] = packed.astype(BF16)

    def a_copy(step):
        to = row[step] + x
        return pltpu.make_async_remote_copy(
            ra.at[z], ra.at[z], a_send, a_recv, device_id={"shard": to}, device_id_type=MESH
        )

    def b_copy(step):
        to = row[0] + column[step]
        return pltpu.make_async_remote_copy(
            rb.at[x], rb.at[x], b_send, b_recv, device_id={"shard": to}, device_id_type=MESH
        )

    def c_copy(step):
        to = other[step]
        return pltpu.make_async_remote_copy(
            rb, rc.at[expert], c_send, c_recv, device_id={"expert": to}, device_id_type=MESH
        )

    def block_copy(p, dz, dx):
        to = row[dz] + column[dx]
        return pltpu.make_async_remote_copy(
            send.at[p, to],
            recv.at[p, shard],
            send_sem.at[p],
            recv_sem.at[p],
            device_id={"shard": to},
            device_id_type=MESH,
        )

    def took(ref, sem):
        pltpu.make_async_copy(ref, ref, sem).wait()

    @pl.loop(0, PAIRS)
    def _(p):
        for copy in loads(p):
            copy.wait()

        @pl.when(p + 2 < PAIRS)
        def _():
            for copy in loads(p + 2):
                copy.start()

        turned = []
        for i in range(2):
            e = 2 * p + i
            a = jnp.concatenate(
                [mg_v[e] + sg_v[e].astype(F32), mu_v[e] + su_v[e].astype(F32)], axis=0
            )
            turned.append(a.T.reshape(NS, TAKE, 128))
        send[p] = jnp.concatenate(turned, axis=1).astype(BF16)
        recv[p, shard] = send[p, shard]

        @pl.when(p == 0)
        def _():
            pl.semaphore_wait(barrier, NS - 1 + NE - 1)

            for step in range(1, NZ):
                a_copy(step).start()

        @pl.when(p == 2)
        def _():
            took(ra.at[pl.ds(0, NZ - 1)], a_recv)
            rb[x] = ra[...].astype(F32).reshape(8 * NZ, 128).astype(BF16)

            for step in range(1, NX):
                b_copy(step).start()

        @pl.when(p == 4)
        def _():
            took(rb.at[pl.ds(0, NX - 1)], b_recv)
            rc[expert] = rb[...]

            for step in range(1, NE):
                c_copy(step).start()

        for dz, dx in OFFSETS:
            block_copy(p, dz, dx).start()

    def merge(p):
        took(recv.at[p, pl.ds(0, NS - 1)], recv_sem.at[p])
        low = lax.broadcasted_iota(jnp.int32, (BLOCK, 128), 1) < 64
        for j in range(NS // 2):
            a, b = recv[p, 2 * j].astype(F32), recv[p, 2 * j + 1].astype(F32)
            g = jnp.where(low, a, pltpu.roll(b, 64, 1))
            u = jnp.where(low, pltpu.roll(a, 64, 1), b)
            for i in range(2):
                rows = slice(TAKE * i, TAKE * (i + 1))
                gate[2 * p + i, :, 128 * j : 128 * (j + 1)] = g[rows].astype(BF16)
                up[2 * p + i, :, 128 * j : 128 * (j + 1)] = u[rows].astype(BF16)

    @pl.loop(0, PAIRS // 2)
    def _(p):
        merge(p)

    took(rc.at[pl.ds(0, NE - 1)], c_recv)
    lane = lax.broadcasted_iota(jnp.int32, (8, 128), 1) // 16

    @pl.loop(0, NX)
    def _(i):
        @pl.loop(0, NZ // 2)
        def _(h):
            total = [[None] * 8, [None] * 8]
            for e in range(NE):
                both = rc[e, i, pl.ds(pl.multiple_of(16 * h, 16), 16), :].astype(F32)
                for q in range(2):
                    one = both[8 * q : 8 * q + 8]
                    for k in range(8):
                        turn = 16 * ((e - k) % 8)
                        moved = pltpu.roll(one, turn, 1) if turn else one
                        old = total[q][k]
                        total[q][k] = moved if old is None else jnp.where(lane == e, moved, old)
            for q in range(2):
                row = pl.multiple_of(((2 * h + q) * NX + i) * ROWS, ROWS)
                router[pl.ds(row, ROWS), :] = jnp.concatenate(total[q], axis=0).astype(BF16)

    @pl.loop(PAIRS // 2, PAIRS)
    def _(p):
        merge(p)

    @pl.loop(0, PAIRS)
    def _(p):
        took(send.at[p, pl.ds(0, NS - 1)], send_sem.at[p])

    took(ra.at[pl.ds(0, NZ - 1)], a_send)
    took(rb.at[pl.ds(0, NX - 1)], b_send)
    took(rc.at[pl.ds(0, NE - 1)], c_send)


def store(gate, up, router, gate_out, up_out, router_out, sem):
    copies = []
    for src, dst in ((gate, gate_out), (up, up_out), (router, router_out)):
        size = src.shape[0] // PIECES
        for k in range(PIECES):
            at = pl.ds(size * k, size)
            copies.append(pltpu.make_async_copy(src.at[at], dst.at[at], sem.at[len(copies)]))
    for copy in copies:
        copy.start()
    for copy in copies:
        copy.wait()


def shards(master_gate, second_gate, master_up, second_up, router_weight, router_gain):
    dma = pltpu.SemaphoreType.DMA
    hbm, vmem = pl.BlockSpec(memory_space=pltpu.HBM), pl.BlockSpec(memory_space=pltpu.VMEM)
    shapes = (
        jax.ShapeDtypeStruct((E, TAKE, NS * ROWS), BF16),
        jax.ShapeDtypeStruct((E, TAKE, NS * ROWS), BF16),
        jax.ShapeDtypeStruct((NS * ROWS, 16 * NE), BF16),
    )
    held = pl.pallas_call(
        exchange,
        out_shape=shapes,
        in_specs=[hbm] * 6,
        out_specs=(vmem,) * 3,
        scratch_shapes=[
            pltpu.VMEM((E, ROWS, COLS), F32),
            pltpu.VMEM((E, ROWS, COLS), BF16),
            pltpu.VMEM((E, ROWS, COLS), F32),
            pltpu.VMEM((E, ROWS, COLS), BF16),
            pltpu.VMEM((16, ROWS), F32),
            pltpu.VMEM((1, ROWS), F32),
            pltpu.VMEM((128, 128), F32),
            pltpu.VMEM((PAIRS, NS, BLOCK, 128), BF16),
            pltpu.VMEM((PAIRS, NS, BLOCK, 128), BF16),
            pltpu.VMEM((NZ, 8, 128), BF16),
            pltpu.VMEM((NX, 8 * NZ, 128), BF16),
            pltpu.VMEM((NE, NX, 8 * NZ, 128), BF16),
            dma((4, PAIRS)),
            dma((2,)),
            dma((PAIRS,)),
            dma((PAIRS,)),
        ]
        + [dma] * 6,
        compiler_params=pltpu.CompilerParams(
            collective_id=0, has_side_effects=True, vmem_limit_bytes=30 << 20
        ),
        name="exchange",
    )(
        *(
            pltpu.with_memory_space_constraint(a, pltpu.HBM)
            for a in (
                master_gate, second_gate, master_up, second_up,
                router_weight.T, router_gain.reshape(1, ROWS),
            )
        )
    )
    return pl.pallas_call(
        store,
        out_shape=shapes,
        in_specs=[vmem] * 3,
        out_specs=(hbm,) * 3,
        scratch_shapes=[dma((3 * PIECES,))],
        compiler_params=pltpu.CompilerParams(vmem_limit_bytes=8 << 20),
        name="store",
    )(*held)


def solution(mesh):
    in_specs = (P("expert", "shard", None),) * 4 + (P("shard", "expert"), P("shard"))
    out_specs = (P("expert", "shard", None), P("expert", "shard", None), P())
    return jax.shard_map(shards, mesh=mesh, in_specs=in_specs, out_specs=out_specs, check_vma=False)
```

```python
import jax
import jax.numpy as jnp
from jax import lax
from jax.experimental import pallas as pl
from jax.experimental.pallas import tpu as pltpu
from jax.sharding import PartitionSpec as P

MESH = pl.DeviceIdType.MESH
NZ, NX = 8, 4
NS = NZ * NX
NE = 8
E = 16
PAIRS = E // 2
ROWS = 64
COLS = 768
TAKE = COLS // NS
BLOCK = 2 * TAKE
F32, BF16 = jnp.float32, jnp.bfloat16
NEAR = [(dz, dx) for dz in (1, 7, 0) for dx in (2, 1, 3, 0) if dz or dx]
FAR = [(dz, dx) for dz in (4, 3, 5, 2, 6) for dx in (2, 1, 3, 0)]
MID = 1


def merged(blocks, gate, up):
    low = lax.broadcasted_iota(jnp.int32, (BLOCK, 128), 1) < 64
    for j in range(NS // 2):
        a, b = blocks[2 * j].astype(F32), blocks[2 * j + 1].astype(F32)
        g = jnp.where(low, a, pltpu.roll(b, 64, 1))
        u = jnp.where(low, pltpu.roll(a, 64, 1), b)
        for i in range(2):
            rows = slice(TAKE * i, TAKE * (i + 1))
            gate[i, :, 128 * j : 128 * (j + 1)] = g[rows].astype(BF16)
            up[i, :, 128 * j : 128 * (j + 1)] = u[rows].astype(BF16)


def exchange(
    mg, sg, mu, su, rw, rg,
    gate, up, router, recv,
    mg_v, sg_v, mu_v, su_v, rw_v, rg_v, wide, send, ra, rb, rc,
    load_sem, small_sem, send_sem, recv_sem, near_sem, mid_sem, open_sem, all_sem, a_send, a_recv, b_send, b_recv, c_send, c_recv,
):
    shard, expert = lax.axis_index("shard"), lax.axis_index("expert")
    z, x = shard // NX, shard % NX
    row = [lax.rem(z + k, NZ) * NX for k in range(NZ)]
    column = [lax.rem(x + k, NX) for k in range(NX)]
    other = [lax.rem(expert + k, NE) for k in range(NE)]

    def loads(p):
        at = pl.ds(2 * p, 2)
        return [
            pltpu.make_async_copy(src.at[at], dst.at[at], load_sem.at[k, p])
            for k, (src, dst) in enumerate(((mg, mg_v), (sg, sg_v), (mu, mu_v), (su, su_v)))
        ]

    for copy in loads(0):
        copy.start()
    small = (
        pltpu.make_async_copy(rw, rw_v, small_sem.at[0]),
        pltpu.make_async_copy(rg, rg_v, small_sem.at[1]),
    )
    for copy in small:
        copy.start()

    barrier = pltpu.get_barrier_semaphore()

    for dz, dx in NEAR:
        to = row[dz] + column[dx]
        pl.semaphore_signal(barrier, 1, device_id={"shard": to}, device_id_type=MESH)

    @pl.when(shard == 0)
    def _():
        for k in range(1, NE):
            pl.semaphore_signal(barrier, 1, device_id={"expert": other[k]}, device_id_type=MESH)

    for copy in loads(1):
        copy.start()

    def a_copy(step):
        to = row[step] + x
        return pltpu.make_async_remote_copy(
            ra.at[z], ra.at[z], a_send, a_recv, device_id={"shard": to}, device_id_type=MESH
        )

    def b_copy(step):
        to = row[0] + column[step]
        return pltpu.make_async_remote_copy(
            rb.at[x], rb.at[x], b_send, b_recv, device_id={"shard": to}, device_id_type=MESH
        )

    def c_copy(step):
        to = other[step]
        return pltpu.make_async_remote_copy(
            rb, rc.at[expert], c_send, c_recv, device_id={"expert": to}, device_id_type=MESH
        )

    def block_copy(p, dz, dx):
        to = row[dz] + column[dx]
        return pltpu.make_async_remote_copy(
            send.at[p, to],
            recv.at[p, shard],
            send_sem.at[p],
            recv_sem.at[p],
            device_id={"shard": to},
            device_id_type=MESH,
        )

    def tell(sem, step):
        for dz in (step, NZ - step):
            pl.semaphore_signal(sem, 1, device_id={"shard": row[dz] + x}, device_id_type=MESH)

    def took(ref, sem):
        pltpu.make_async_copy(ref, ref, sem).wait()

    @pl.loop(0, PAIRS)
    def _(p):
        for copy in loads(p):
            copy.wait()

        @pl.when(p + 2 < PAIRS)
        def _():
            for copy in loads(p + 2):
                copy.start()

        turned = []
        for i in range(2):
            e = 2 * p + i
            a = jnp.concatenate(
                [mg_v[e] + sg_v[e].astype(F32), mu_v[e] + su_v[e].astype(F32)], axis=0
            )
            turned.append(a.T.reshape(NS, TAKE, 128))
        send[p] = jnp.concatenate(turned, axis=1).astype(BF16)
        recv[p, shard] = send[p, shard]

        @pl.when(p == 0)
        def _():
            pl.semaphore_wait(barrier, len(NEAR) + jnp.where(shard == 0, NE - 1, 0))
            tell(near_sem, 1)

        for dz, dx in NEAR:
            block_copy(p, dz, dx).start()

        @pl.when(p == 0)
        def _():
            for copy in small:
                copy.wait()
            wide[...] = jnp.zeros((128, 128), F32)
            wide[0:16, 0:ROWS] = (rw_v[...] * rg_v[...]).astype(BF16).astype(F32)
            tall = wide[...].T
            packed = tall[0:8]
            for k in range(1, 8):
                packed = packed + pltpu.roll(tall[8 * k : 8 * k + 8], 16 * k, 1)
            ra[z] = packed.astype(BF16)

        @pl.when(p == MID)
        def _():
            pl.semaphore_wait(near_sem, 2)
            tell(mid_sem, 2)

    pl.semaphore_wait(mid_sem, 2)

    @pl.when(shard == 0)
    def _():
        for k in range(1, NE):
            pl.semaphore_signal(open_sem, 1, device_id={"expert": other[k]}, device_id_type=MESH)

    for step in range(1, NZ):
        a_copy(step).start()

    @pl.loop(0, PAIRS)
    def _(p):
        for dz, dx in FAR:
            block_copy(p, dz, dx).start()

        @pl.when(p == 1)
        def _():
            took(ra.at[pl.ds(0, NZ - 1)], a_recv)
            rb[x] = ra[...].astype(F32).reshape(8 * NZ, 128).astype(BF16)
            for step in range(1, NX):
                b_copy(step).start()

        @pl.when((p == 2) & (shard == 0))
        def _():
            pl.semaphore_wait(open_sem, NE - 1)
            for dz, dx in NEAR + FAR:
                to = row[dz] + column[dx]
                pl.semaphore_signal(all_sem, 1, device_id={"shard": to}, device_id_type=MESH)

        @pl.when((p == 3) & (shard != 0))
        def _():
            pl.semaphore_wait(all_sem, 1)

        @pl.when(p == 3)
        def _():
            took(rb.at[pl.ds(0, NX - 1)], b_recv)
            rc[expert] = rb[...]
            for step in range(1, NE):
                c_copy(step).start()

    def merge(p):
        took(recv.at[p, pl.ds(0, NS - 1)], recv_sem.at[p])
        merged(recv.at[p], gate.at[pl.ds(2 * p, 2)], up.at[pl.ds(2 * p, 2)])

    @pl.loop(0, PAIRS // 2)
    def _(p):
        merge(p)

    took(rc.at[pl.ds(0, NE - 1)], c_recv)
    lane = lax.broadcasted_iota(jnp.int32, (8, 128), 1) // 16

    @pl.loop(0, NX)
    def _(i):
        @pl.loop(0, NZ // 2)
        def _(h):
            total = [[None] * 8, [None] * 8]
            for e in range(NE):
                both = rc[e, i, pl.ds(pl.multiple_of(16 * h, 16), 16), :].astype(F32)
                for q in range(2):
                    one = both[8 * q : 8 * q + 8]
                    for k in range(8):
                        turn = 16 * ((e - k) % 8)
                        moved = pltpu.roll(one, turn, 1) if turn else one
                        old = total[q][k]
                        total[q][k] = moved if old is None else jnp.where(lane == e, moved, old)
            for q in range(2):
                row = pl.multiple_of(((2 * h + q) * NX + i) * ROWS, ROWS)
                router[pl.ds(row, ROWS), :] = jnp.concatenate(total[q], axis=0).astype(BF16)

    @pl.loop(PAIRS // 2, PAIRS - 1)
    def _(p):
        merge(p)

    took(recv.at[PAIRS - 1, pl.ds(0, NS - 1)], recv_sem.at[PAIRS - 1])

    @pl.loop(0, PAIRS)
    def _(p):
        took(send.at[p, pl.ds(0, NS - 1)], send_sem.at[p])

    took(ra.at[pl.ds(0, NZ - 1)], a_send)
    took(rb.at[pl.ds(0, NX - 1)], b_send)
    took(rc.at[pl.ds(0, NE - 1)], c_send)


def store(gate, up, router, recv, gate_out, up_out, router_out, gate_v, up_v, sem):
    first, last = pl.ds(0, E - 2), pl.ds(E - 2, 2)
    copies = [
        pltpu.make_async_copy(src, dst, sem.at[k])
        for k, (src, dst) in enumerate(
            (
                (gate, gate_out.at[first]),
                (up, up_out.at[first]),
                (router, router_out),
                (gate_v, gate_out.at[last]),
                (up_v, up_out.at[last]),
            )
        )
    ]
    for copy in copies[:3]:
        copy.start()
    merged(recv.at[PAIRS - 1], gate_v, up_v)
    for copy in copies[3:]:
        copy.start()
    for copy in copies:
        copy.wait()


def shards(master_gate, second_gate, master_up, second_up, router_weight, router_gain):
    dma = pltpu.SemaphoreType.DMA
    hbm, vmem = pl.BlockSpec(memory_space=pltpu.HBM), pl.BlockSpec(memory_space=pltpu.VMEM)
    shapes = (
        jax.ShapeDtypeStruct((E, TAKE, NS * ROWS), BF16),
        jax.ShapeDtypeStruct((E, TAKE, NS * ROWS), BF16),
        jax.ShapeDtypeStruct((NS * ROWS, 16 * NE), BF16),
    )
    part = jax.ShapeDtypeStruct((E - 2, TAKE, NS * ROWS), BF16)
    blocks = jax.ShapeDtypeStruct((PAIRS, NS, BLOCK, 128), BF16)
    held = pl.pallas_call(
        exchange,
        out_shape=(part, part, shapes[2], blocks),
        in_specs=[hbm] * 6,
        out_specs=(vmem,) * 4,
        scratch_shapes=[
            pltpu.VMEM((E, ROWS, COLS), F32),
            pltpu.VMEM((E, ROWS, COLS), BF16),
            pltpu.VMEM((E, ROWS, COLS), F32),
            pltpu.VMEM((E, ROWS, COLS), BF16),
            pltpu.VMEM((16, ROWS), F32),
            pltpu.VMEM((1, ROWS), F32),
            pltpu.VMEM((128, 128), F32),
            pltpu.VMEM((PAIRS, NS, BLOCK, 128), BF16),
            pltpu.VMEM((NZ, 8, 128), BF16),
            pltpu.VMEM((NX, 8 * NZ, 128), BF16),
            pltpu.VMEM((NE, NX, 8 * NZ, 128), BF16),
            dma((4, PAIRS)),
            dma((2,)),
            dma((PAIRS,)),
            dma((PAIRS,)),
        ]
        + [pltpu.SemaphoreType.REGULAR] * 4
        + [dma] * 6,
        compiler_params=pltpu.CompilerParams(
            collective_id=0, has_side_effects=True, vmem_limit_bytes=30 << 20
        ),
        name="exchange",
    )(
        *(
            pltpu.with_memory_space_constraint(a, pltpu.HBM)
            for a in (
                master_gate, second_gate, master_up, second_up,
                router_weight.T, router_gain.reshape(1, ROWS),
            )
        )
    )
    return pl.pallas_call(
        store,
        out_shape=shapes,
        in_specs=[vmem] * 4,
        out_specs=(hbm,) * 3,
        scratch_shapes=[pltpu.VMEM((2, TAKE, NS * ROWS), BF16)] * 2 + [dma((5,))],
        compiler_params=pltpu.CompilerParams(vmem_limit_bytes=8 << 20),
        name="store",
    )(*held)


def solution(mesh):
    in_specs = (P("expert", "shard", None),) * 4 + (P("shard", "expert"), P("shard"))
    out_specs = (P("expert", "shard", None), P("expert", "shard", None), P())
    return jax.shard_map(shards, mesh=mesh, in_specs=in_specs, out_specs=out_specs, check_vma=False)
```

```python
import jax
import jax.numpy as jnp
from jax import lax
from jax.experimental import pallas as pl
from jax.experimental.pallas import tpu as pltpu
from jax.sharding import PartitionSpec as P

MESH = pl.DeviceIdType.MESH
NZ, NX = 8, 4
NS = NZ * NX
NE = 8
E = 16
PAIRS = E // 2
ROWS = 64
COLS = 768
TAKE = COLS // NS
BLOCK = 2 * TAKE
F32, BF16 = jnp.float32, jnp.bfloat16
NEAR = [(dz, dx) for dz in (1, 7, 0) for dx in (2, 1, 3, 0) if dz or dx]
FAR = [(dz, dx) for dz in (4, 3, 5, 2, 6) for dx in (2, 1, 3, 0)]
EARLY = 5
MID = 2


def merged(blocks, gate, up):
    low = lax.broadcasted_iota(jnp.int32, (BLOCK, 128), 1) < 64
    for j in range(NS // 2):
        a, b = blocks[2 * j].astype(F32), blocks[2 * j + 1].astype(F32)
        g = jnp.where(low, a, pltpu.roll(b, 64, 1))
        u = jnp.where(low, pltpu.roll(a, 64, 1), b)
        for i in range(2):
            rows = slice(TAKE * i, TAKE * (i + 1))
            gate[i, :, 128 * j : 128 * (j + 1)] = g[rows].astype(BF16)
            up[i, :, 128 * j : 128 * (j + 1)] = u[rows].astype(BF16)


def exchange(
    mg, sg, mu, su, rw, rg,
    gate, up, router, recv,
    mg_v, sg_v, mu_v, su_v, rw_v, rg_v, wide, send, ra, rb, rc,
    load_sem, small_sem, send_sem, recv_sem, near_sem, mid_sem, open_sem, all_sem, a_send, a_recv, b_send, b_recv, c_send, c_recv,
):
    shard, expert = lax.axis_index("shard"), lax.axis_index("expert")
    z, x = shard // NX, shard % NX
    row = [lax.rem(z + k, NZ) * NX for k in range(NZ)]
    column = [lax.rem(x + k, NX) for k in range(NX)]
    other = [lax.rem(expert + k, NE) for k in range(NE)]

    def loads(p):
        at = pl.ds(2 * p, 2)
        return [
            pltpu.make_async_copy(src.at[at], dst.at[at], load_sem.at[k, p])
            for k, (src, dst) in enumerate(((mg, mg_v), (sg, sg_v), (mu, mu_v), (su, su_v)))
        ]

    for copy in loads(0):
        copy.start()
    small = (
        pltpu.make_async_copy(rw, rw_v, small_sem.at[0]),
        pltpu.make_async_copy(rg, rg_v, small_sem.at[1]),
    )
    for copy in small:
        copy.start()

    barrier = pltpu.get_barrier_semaphore()

    for dz, dx in NEAR:
        to = row[dz] + column[dx]
        pl.semaphore_signal(barrier, 1, device_id={"shard": to}, device_id_type=MESH)

    @pl.when(shard == 0)
    def _():
        for k in range(1, NE):
            pl.semaphore_signal(barrier, 1, device_id={"expert": other[k]}, device_id_type=MESH)

    for copy in loads(1):
        copy.start()

    def a_copy(step):
        to = row[step] + x
        return pltpu.make_async_remote_copy(
            ra.at[z], ra.at[z], a_send, a_recv, device_id={"shard": to}, device_id_type=MESH
        )

    def b_copy(step):
        to = row[0] + column[step]
        return pltpu.make_async_remote_copy(
            rb.at[x], rb.at[x], b_send, b_recv, device_id={"shard": to}, device_id_type=MESH
        )

    def c_copy(step):
        to = other[step]
        return pltpu.make_async_remote_copy(
            rb, rc.at[expert], c_send, c_recv, device_id={"expert": to}, device_id_type=MESH
        )

    def block_copy(p, dz, dx):
        to = row[dz] + column[dx]
        return pltpu.make_async_remote_copy(
            send.at[p, to],
            recv.at[p, shard],
            send_sem.at[p],
            recv_sem.at[p],
            device_id={"shard": to},
            device_id_type=MESH,
        )

    def tell(sem, step):
        for dz in (step, NZ - step):
            pl.semaphore_signal(sem, 1, device_id={"shard": row[dz] + x}, device_id_type=MESH)

    def took(ref, sem):
        pltpu.make_async_copy(ref, ref, sem).wait()

    @pl.loop(0, PAIRS)
    def _(p):
        for copy in loads(p):
            copy.wait()

        @pl.when(p + 2 < PAIRS)
        def _():
            for copy in loads(p + 2):
                copy.start()

        turned = []
        for i in range(2):
            e = 2 * p + i
            a = jnp.concatenate(
                [mg_v[e] + sg_v[e].astype(F32), mu_v[e] + su_v[e].astype(F32)], axis=0
            )
            turned.append(a.T.reshape(NS, TAKE, 128))
        send[p] = jnp.concatenate(turned, axis=1).astype(BF16)
        recv[p, shard] = send[p, shard]

        @pl.when(p == 0)
        def _():
            pl.semaphore_wait(barrier, len(NEAR) + jnp.where(shard == 0, NE - 1, 0))
            tell(near_sem, 1)

        @pl.when(p < EARLY)
        def _():
            for dz, dx in NEAR:
                block_copy(p, dz, dx).start()

        @pl.when(p == 0)
        def _():
            for copy in small:
                copy.wait()
            wide[...] = jnp.zeros((128, 128), F32)
            wide[0:16, 0:ROWS] = (rw_v[...] * rg_v[...]).astype(BF16).astype(F32)
            tall = wide[...].T
            packed = tall[0:8]
            for k in range(1, 8):
                packed = packed + pltpu.roll(tall[8 * k : 8 * k + 8], 16 * k, 1)
            ra[z] = packed.astype(BF16)

        @pl.when(p == MID)
        def _():
            pl.semaphore_wait(near_sem, 2)
            tell(mid_sem, 2)

    pl.semaphore_wait(mid_sem, 2)

    @pl.when(shard == 0)
    def _():
        for k in range(1, NE):
            pl.semaphore_signal(open_sem, 1, device_id={"expert": other[k]}, device_id_type=MESH)

    for step in range(1, NZ):
        a_copy(step).start()

    @pl.loop(0, PAIRS)
    def _(p):
        for dz, dx in FAR:
            block_copy(p, dz, dx).start()

        @pl.when(p >= EARLY)
        def _():
            for dz, dx in NEAR:
                block_copy(p, dz, dx).start()

        @pl.when(p == 1)
        def _():
            took(ra.at[pl.ds(0, NZ - 1)], a_recv)
            rb[x] = ra[...].astype(F32).reshape(8 * NZ, 128).astype(BF16)
            for step in range(1, NX):
                b_copy(step).start()

        @pl.when((p == 2) & (shard == 0))
        def _():
            pl.semaphore_wait(open_sem, NE - 1)
            for dz, dx in NEAR + FAR:
                to = row[dz] + column[dx]
                pl.semaphore_signal(all_sem, 1, device_id={"shard": to}, device_id_type=MESH)

        @pl.when((p == 3) & (shard != 0))
        def _():
            pl.semaphore_wait(all_sem, 1)

        @pl.when(p == 3)
        def _():
            took(rb.at[pl.ds(0, NX - 1)], b_recv)
            rc[expert] = rb[...]
            for step in range(1, NE):
                c_copy(step).start()

    def merge(p):
        took(recv.at[p, pl.ds(0, NS - 1)], recv_sem.at[p])
        merged(recv.at[p], gate.at[pl.ds(2 * p, 2)], up.at[pl.ds(2 * p, 2)])

    @pl.loop(0, PAIRS // 2)
    def _(p):
        merge(p)

    took(rc.at[pl.ds(0, NE - 1)], c_recv)
    lane = lax.broadcasted_iota(jnp.int32, (8, 128), 1) // 16

    @pl.loop(0, NX)
    def _(i):
        @pl.loop(0, NZ // 2)
        def _(h):
            total = [[None] * 8, [None] * 8]
            for e in range(NE):
                both = rc[e, i, pl.ds(pl.multiple_of(16 * h, 16), 16), :].astype(F32)
                for q in range(2):
                    one = both[8 * q : 8 * q + 8]
                    for k in range(8):
                        turn = 16 * ((e - k) % 8)
                        moved = pltpu.roll(one, turn, 1) if turn else one
                        old = total[q][k]
                        total[q][k] = moved if old is None else jnp.where(lane == e, moved, old)
            for q in range(2):
                row = pl.multiple_of(((2 * h + q) * NX + i) * ROWS, ROWS)
                router[pl.ds(row, ROWS), :] = jnp.concatenate(total[q], axis=0).astype(BF16)

    @pl.loop(PAIRS // 2, PAIRS - 1)
    def _(p):
        merge(p)

    took(recv.at[PAIRS - 1, pl.ds(0, NS - 1)], recv_sem.at[PAIRS - 1])

    @pl.loop(0, PAIRS)
    def _(p):
        took(send.at[p, pl.ds(0, NS - 1)], send_sem.at[p])

    took(ra.at[pl.ds(0, NZ - 1)], a_send)
    took(rb.at[pl.ds(0, NX - 1)], b_send)
    took(rc.at[pl.ds(0, NE - 1)], c_send)


def store(gate, up, router, recv, gate_out, up_out, router_out, gate_v, up_v, sem):
    first, last = pl.ds(0, E - 2), pl.ds(E - 2, 2)
    copies = [
        pltpu.make_async_copy(src, dst, sem.at[k])
        for k, (src, dst) in enumerate(
            (
                (gate, gate_out.at[first]),
                (up, up_out.at[first]),
                (router, router_out),
                (gate_v, gate_out.at[last]),
                (up_v, up_out.at[last]),
            )
        )
    ]
    for copy in copies[:3]:
        copy.start()
    merged(recv.at[PAIRS - 1], gate_v, up_v)
    for copy in copies[3:]:
        copy.start()
    for copy in copies:
        copy.wait()


def shards(master_gate, second_gate, master_up, second_up, router_weight, router_gain):
    dma = pltpu.SemaphoreType.DMA
    hbm, vmem = pl.BlockSpec(memory_space=pltpu.HBM), pl.BlockSpec(memory_space=pltpu.VMEM)
    shapes = (
        jax.ShapeDtypeStruct((E, TAKE, NS * ROWS), BF16),
        jax.ShapeDtypeStruct((E, TAKE, NS * ROWS), BF16),
        jax.ShapeDtypeStruct((NS * ROWS, 16 * NE), BF16),
    )
    part = jax.ShapeDtypeStruct((E - 2, TAKE, NS * ROWS), BF16)
    blocks = jax.ShapeDtypeStruct((PAIRS, NS, BLOCK, 128), BF16)
    held = pl.pallas_call(
        exchange,
        out_shape=(part, part, shapes[2], blocks),
        in_specs=[hbm] * 6,
        out_specs=(vmem,) * 4,
        scratch_shapes=[
            pltpu.VMEM((E, ROWS, COLS), F32),
            pltpu.VMEM((E, ROWS, COLS), BF16),
            pltpu.VMEM((E, ROWS, COLS), F32),
            pltpu.VMEM((E, ROWS, COLS), BF16),
            pltpu.VMEM((16, ROWS), F32),
            pltpu.VMEM((1, ROWS), F32),
            pltpu.VMEM((128, 128), F32),
            pltpu.VMEM((PAIRS, NS, BLOCK, 128), BF16),
            pltpu.VMEM((NZ, 8, 128), BF16),
            pltpu.VMEM((NX, 8 * NZ, 128), BF16),
            pltpu.VMEM((NE, NX, 8 * NZ, 128), BF16),
            dma((4, PAIRS)),
            dma((2,)),
            dma((PAIRS,)),
            dma((PAIRS,)),
        ]
        + [pltpu.SemaphoreType.REGULAR] * 4
        + [dma] * 6,
        compiler_params=pltpu.CompilerParams(
            collective_id=0, has_side_effects=True, vmem_limit_bytes=30 << 20
        ),
        name="exchange",
    )(
        *(
            pltpu.with_memory_space_constraint(a, pltpu.HBM)
            for a in (
                master_gate, second_gate, master_up, second_up,
                router_weight.T, router_gain.reshape(1, ROWS),
            )
        )
    )
    return pl.pallas_call(
        store,
        out_shape=shapes,
        in_specs=[vmem] * 4,
        out_specs=(hbm,) * 3,
        scratch_shapes=[pltpu.VMEM((2, TAKE, NS * ROWS), BF16)] * 2 + [dma((5,))],
        compiler_params=pltpu.CompilerParams(vmem_limit_bytes=8 << 20),
        name="store",
    )(*held)


def solution(mesh):
    in_specs = (P("expert", "shard", None),) * 4 + (P("shard", "expert"), P("shard"))
    out_specs = (P("expert", "shard", None), P("expert", "shard", None), P())
    return jax.shard_map(shards, mesh=mesh, in_specs=in_specs, out_specs=out_specs, check_vma=False)
```

```python
import jax
import jax.numpy as jnp
from jax import lax
from jax.experimental import pallas as pl
from jax.experimental.pallas import tpu as pltpu
from jax.sharding import PartitionSpec as P

MESH = pl.DeviceIdType.MESH
NZ, NX = 8, 4
NS = NZ * NX
NE = 8
E = 16
PAIRS = E // 2
ROWS = 64
COLS = 768
TAKE = COLS // NS
BLOCK = 2 * TAKE
F32, BF16 = jnp.float32, jnp.bfloat16
NEAR = [(dz, dx) for dz in (1, 7, 0) for dx in (2, 1, 3, 0) if dz or dx]
FAR = [(dz, dx) for dz in (4, 3, 5, 2, 6) for dx in (2, 1, 3, 0)]
EARLY = 5
SORTED = 5
MID = 2


def merged(blocks, gate, up):
    low = lax.broadcasted_iota(jnp.int32, (BLOCK, 128), 1) < 64
    for j in range(NS // 2):
        a, b = blocks[2 * j].astype(F32), blocks[2 * j + 1].astype(F32)
        g = jnp.where(low, a, pltpu.roll(b, 64, 1))
        u = jnp.where(low, pltpu.roll(a, 64, 1), b)
        for i in range(2):
            rows = slice(TAKE * i, TAKE * (i + 1))
            gate[i, :, 128 * j : 128 * (j + 1)] = g[rows].astype(BF16)
            up[i, :, 128 * j : 128 * (j + 1)] = u[rows].astype(BF16)


def exchange(
    mg, sg, mu, su, rw, rg,
    gate, up, router, recv,
    mg_v, sg_v, mu_v, su_v, rw_v, rg_v, wide, send, ra, rb, rc,
    load_sem, small_sem, send_sem, recv_sem, near_sem, mid_sem, open_sem, all_sem, a_send, a_recv, b_send, b_recv, c_send, c_recv,
):
    shard, expert = lax.axis_index("shard"), lax.axis_index("expert")
    z, x = shard // NX, shard % NX
    row = [lax.rem(z + k, NZ) * NX for k in range(NZ)]
    column = [lax.rem(x + k, NX) for k in range(NX)]
    other = [lax.rem(expert + k, NE) for k in range(NE)]

    def loads(p):
        at = pl.ds(2 * p, 2)
        return [
            pltpu.make_async_copy(src.at[at], dst.at[at], load_sem.at[k, p])
            for k, (src, dst) in enumerate(((mg, mg_v), (sg, sg_v), (mu, mu_v), (su, su_v)))
        ]

    for copy in loads(0):
        copy.start()
    small = (
        pltpu.make_async_copy(rw, rw_v, small_sem.at[0]),
        pltpu.make_async_copy(rg, rg_v, small_sem.at[1]),
    )
    for copy in small:
        copy.start()

    barrier = pltpu.get_barrier_semaphore()

    for dz, dx in NEAR:
        to = row[dz] + column[dx]
        pl.semaphore_signal(barrier, 1, device_id={"shard": to}, device_id_type=MESH)

    @pl.when(shard == 0)
    def _():
        for k in range(1, NE):
            pl.semaphore_signal(barrier, 1, device_id={"expert": other[k]}, device_id_type=MESH)

    for copy in loads(1):
        copy.start()

    def a_copy(step):
        to = row[step] + x
        return pltpu.make_async_remote_copy(
            ra.at[z], ra.at[z], a_send, a_recv, device_id={"shard": to}, device_id_type=MESH
        )

    def b_copy(step):
        to = row[0] + column[step]
        return pltpu.make_async_remote_copy(
            rb.at[x], rb.at[x], b_send, b_recv, device_id={"shard": to}, device_id_type=MESH
        )

    def c_copy(step):
        to = other[step]
        return pltpu.make_async_remote_copy(
            rb, rc.at[expert], c_send, c_recv, device_id={"expert": to}, device_id_type=MESH
        )

    def block_copy(p, dz, dx):
        to = row[dz] + column[dx]
        return pltpu.make_async_remote_copy(
            send.at[p, to],
            recv.at[p, shard],
            send_sem.at[p],
            recv_sem.at[p],
            device_id={"shard": to},
            device_id_type=MESH,
        )

    def tell(sem, step):
        for dz in (step, NZ - step):
            pl.semaphore_signal(sem, 1, device_id={"shard": row[dz] + x}, device_id_type=MESH)

    def took(ref, sem):
        pltpu.make_async_copy(ref, ref, sem).wait()

    @pl.loop(0, PAIRS)
    def _(p):
        for copy in loads(p):
            copy.wait()

        @pl.when(p + 2 < PAIRS)
        def _():
            for copy in loads(p + 2):
                copy.start()

        turned = []
        for i in range(2):
            e = 2 * p + i
            a = jnp.concatenate(
                [mg_v[e] + sg_v[e].astype(F32), mu_v[e] + su_v[e].astype(F32)], axis=0
            )
            turned.append(a.T.reshape(NS, TAKE, 128))
        send[p] = jnp.concatenate(turned, axis=1).astype(BF16)
        recv[p, shard] = send[p, shard]

        @pl.when(p == 0)
        def _():
            pl.semaphore_wait(barrier, len(NEAR) + jnp.where(shard == 0, NE - 1, 0))
            tell(near_sem, 1)

        @pl.when(p < EARLY)
        def _():
            for dz, dx in NEAR:
                block_copy(p, dz, dx).start()

        @pl.when(p == 0)
        def _():
            for copy in small:
                copy.wait()
            wide[...] = jnp.zeros((128, 128), F32)
            wide[0:16, 0:ROWS] = (rw_v[...] * rg_v[...]).astype(BF16).astype(F32)
            tall = wide[...].T
            packed = tall[0:8]
            for k in range(1, 8):
                packed = packed + pltpu.roll(tall[8 * k : 8 * k + 8], 16 * k, 1)
            ra[z] = packed.astype(BF16)

        @pl.when(p == MID)
        def _():
            pl.semaphore_wait(near_sem, 2)
            tell(mid_sem, 2)

    pl.semaphore_wait(mid_sem, 2)

    @pl.when(shard == 0)
    def _():
        for k in range(1, NE):
            pl.semaphore_signal(open_sem, 1, device_id={"expert": other[k]}, device_id_type=MESH)

    for step in range(1, NZ):
        a_copy(step).start()

    @pl.loop(0, PAIRS)
    def _(p):
        @pl.when(p < SORTED)
        def _():
            for dz, dx in FAR:
                block_copy(p, dz, dx).start()

        @pl.when((p >= EARLY) & (p < SORTED))
        def _():
            for dz, dx in NEAR:
                block_copy(p, dz, dx).start()

        @pl.when(p >= SORTED)
        def _():
            for first in (True, False):
                for dz in (4, 3, 5, 2, 6, 1, 7, 0):

                    @pl.when((row[dz] < NX * 2) == first)
                    def _():
                        for dx in (2, 1, 3, 0) if dz else (2, 1, 3):
                            block_copy(p, dz, dx).start()

        @pl.when(p == 1)
        def _():
            took(ra.at[pl.ds(0, NZ - 1)], a_recv)
            rb[x] = ra[...].astype(F32).reshape(8 * NZ, 128).astype(BF16)
            for step in range(1, NX):
                b_copy(step).start()

        @pl.when((p == 2) & (shard == 0))
        def _():
            pl.semaphore_wait(open_sem, NE - 1)
            for dz, dx in NEAR + FAR:
                to = row[dz] + column[dx]
                pl.semaphore_signal(all_sem, 1, device_id={"shard": to}, device_id_type=MESH)

        @pl.when((p == 3) & (shard != 0))
        def _():
            pl.semaphore_wait(all_sem, 1)

        @pl.when(p == 3)
        def _():
            took(rb.at[pl.ds(0, NX - 1)], b_recv)
            rc[expert] = rb[...]
            for step in range(1, NE):
                c_copy(step).start()

    def merge(p):
        took(recv.at[p, pl.ds(0, NS - 1)], recv_sem.at[p])
        merged(recv.at[p], gate.at[pl.ds(2 * p, 2)], up.at[pl.ds(2 * p, 2)])

    @pl.loop(0, PAIRS // 2)
    def _(p):
        merge(p)

    took(rc.at[pl.ds(0, NE - 1)], c_recv)
    lane = lax.broadcasted_iota(jnp.int32, (8, 128), 1) // 16

    @pl.loop(0, NX)
    def _(i):
        @pl.loop(0, NZ // 2)
        def _(h):
            total = [[None] * 8, [None] * 8]
            for e in range(NE):
                both = rc[e, i, pl.ds(pl.multiple_of(16 * h, 16), 16), :].astype(F32)
                for q in range(2):
                    one = both[8 * q : 8 * q + 8]
                    for k in range(8):
                        turn = 16 * ((e - k) % 8)
                        moved = pltpu.roll(one, turn, 1) if turn else one
                        old = total[q][k]
                        total[q][k] = moved if old is None else jnp.where(lane == e, moved, old)
            for q in range(2):
                row = pl.multiple_of(((2 * h + q) * NX + i) * ROWS, ROWS)
                router[pl.ds(row, ROWS), :] = jnp.concatenate(total[q], axis=0).astype(BF16)

    @pl.loop(PAIRS // 2, PAIRS - 1)
    def _(p):
        merge(p)

    took(recv.at[PAIRS - 1, pl.ds(0, NS - 1)], recv_sem.at[PAIRS - 1])

    @pl.loop(0, PAIRS)
    def _(p):
        took(send.at[p, pl.ds(0, NS - 1)], send_sem.at[p])

    took(ra.at[pl.ds(0, NZ - 1)], a_send)
    took(rb.at[pl.ds(0, NX - 1)], b_send)
    took(rc.at[pl.ds(0, NE - 1)], c_send)


def store(gate, up, router, recv, gate_out, up_out, router_out, gate_v, up_v, sem):
    first, last = pl.ds(0, E - 2), pl.ds(E - 2, 2)
    copies = [
        pltpu.make_async_copy(src, dst, sem.at[k])
        for k, (src, dst) in enumerate(
            (
                (gate, gate_out.at[first]),
                (up, up_out.at[first]),
                (router, router_out),
                (gate_v, gate_out.at[last]),
                (up_v, up_out.at[last]),
            )
        )
    ]
    for copy in copies[:3]:
        copy.start()
    merged(recv.at[PAIRS - 1], gate_v, up_v)
    for copy in copies[3:]:
        copy.start()
    for copy in copies:
        copy.wait()


def shards(master_gate, second_gate, master_up, second_up, router_weight, router_gain):
    dma = pltpu.SemaphoreType.DMA
    hbm, vmem = pl.BlockSpec(memory_space=pltpu.HBM), pl.BlockSpec(memory_space=pltpu.VMEM)
    shapes = (
        jax.ShapeDtypeStruct((E, TAKE, NS * ROWS), BF16),
        jax.ShapeDtypeStruct((E, TAKE, NS * ROWS), BF16),
        jax.ShapeDtypeStruct((NS * ROWS, 16 * NE), BF16),
    )
    part = jax.ShapeDtypeStruct((E - 2, TAKE, NS * ROWS), BF16)
    blocks = jax.ShapeDtypeStruct((PAIRS, NS, BLOCK, 128), BF16)
    held = pl.pallas_call(
        exchange,
        out_shape=(part, part, shapes[2], blocks),
        in_specs=[hbm] * 6,
        out_specs=(vmem,) * 4,
        scratch_shapes=[
            pltpu.VMEM((E, ROWS, COLS), F32),
            pltpu.VMEM((E, ROWS, COLS), BF16),
            pltpu.VMEM((E, ROWS, COLS), F32),
            pltpu.VMEM((E, ROWS, COLS), BF16),
            pltpu.VMEM((16, ROWS), F32),
            pltpu.VMEM((1, ROWS), F32),
            pltpu.VMEM((128, 128), F32),
            pltpu.VMEM((PAIRS, NS, BLOCK, 128), BF16),
            pltpu.VMEM((NZ, 8, 128), BF16),
            pltpu.VMEM((NX, 8 * NZ, 128), BF16),
            pltpu.VMEM((NE, NX, 8 * NZ, 128), BF16),
            dma((4, PAIRS)),
            dma((2,)),
            dma((PAIRS,)),
            dma((PAIRS,)),
        ]
        + [pltpu.SemaphoreType.REGULAR] * 4
        + [dma] * 6,
        compiler_params=pltpu.CompilerParams(
            collective_id=0, has_side_effects=True, vmem_limit_bytes=30 << 20
        ),
        name="exchange",
    )(
        *(
            pltpu.with_memory_space_constraint(a, pltpu.HBM)
            for a in (
                master_gate, second_gate, master_up, second_up,
                router_weight.T, router_gain.reshape(1, ROWS),
            )
        )
    )
    return pl.pallas_call(
        store,
        out_shape=shapes,
        in_specs=[vmem] * 4,
        out_specs=(hbm,) * 3,
        scratch_shapes=[pltpu.VMEM((2, TAKE, NS * ROWS), BF16)] * 2 + [dma((5,))],
        compiler_params=pltpu.CompilerParams(vmem_limit_bytes=8 << 20),
        name="store",
    )(*held)


def solution(mesh):
    in_specs = (P("expert", "shard", None),) * 4 + (P("shard", "expert"), P("shard"))
    out_specs = (P("expert", "shard", None), P("expert", "shard", None), P())
    return jax.shard_map(shards, mesh=mesh, in_specs=in_specs, out_specs=out_specs, check_vma=False)
```

```python
import jax
import jax.numpy as jnp
from jax import lax
from jax.experimental import pallas as pl
from jax.experimental.pallas import tpu as pltpu
from jax.sharding import PartitionSpec as P

MESH = pl.DeviceIdType.MESH
NZ, NX = 8, 4
NS = NZ * NX
NE = 8
E = 16
PAIRS = E // 2
ROWS = 64
COLS = 768
TAKE = COLS // NS
BLOCK = 2 * TAKE
F32, BF16 = jnp.float32, jnp.bfloat16
NEAR = [(dz, dx) for dz in (1, 7, 0) for dx in (2, 1, 3, 0) if dz or dx]
FAR = [(dz, dx) for dz in (4, 3, 5, 2, 6) for dx in (2, 1, 3, 0)]
EARLY = 5
SORTED = 5
TIERS = ((0, 2), (2, 3), (3, 8))
MID = 2


def merged(blocks, gate, up):
    low = lax.broadcasted_iota(jnp.int32, (BLOCK, 128), 1) < 64
    for j in range(NS // 2):
        a, b = blocks[2 * j].astype(F32), blocks[2 * j + 1].astype(F32)
        g = jnp.where(low, a, pltpu.roll(b, 64, 1))
        u = jnp.where(low, pltpu.roll(a, 64, 1), b)
        for i in range(2):
            rows = slice(TAKE * i, TAKE * (i + 1))
            gate[i, :, 128 * j : 128 * (j + 1)] = g[rows].astype(BF16)
            up[i, :, 128 * j : 128 * (j + 1)] = u[rows].astype(BF16)


def exchange(
    mg, sg, mu, su, rw, rg,
    gate, up, router, recv,
    mg_v, sg_v, mu_v, su_v, rw_v, rg_v, wide, send, ra, rb, rc,
    load_sem, small_sem, send_sem, recv_sem, near_sem, mid_sem, open_sem, all_sem, a_send, a_recv, b_send, b_recv, c_send, c_recv,
):
    shard, expert = lax.axis_index("shard"), lax.axis_index("expert")
    z, x = shard // NX, shard % NX
    row = [lax.rem(z + k, NZ) * NX for k in range(NZ)]
    column = [lax.rem(x + k, NX) for k in range(NX)]
    other = [lax.rem(expert + k, NE) for k in range(NE)]

    def loads(p):
        at = pl.ds(2 * p, 2)
        return [
            pltpu.make_async_copy(src.at[at], dst.at[at], load_sem.at[k, p])
            for k, (src, dst) in enumerate(((mg, mg_v), (sg, sg_v), (mu, mu_v), (su, su_v)))
        ]

    for copy in loads(0):
        copy.start()
    small = (
        pltpu.make_async_copy(rw, rw_v, small_sem.at[0]),
        pltpu.make_async_copy(rg, rg_v, small_sem.at[1]),
    )
    for copy in small:
        copy.start()

    barrier = pltpu.get_barrier_semaphore()

    for dz, dx in NEAR:
        to = row[dz] + column[dx]
        pl.semaphore_signal(barrier, 1, device_id={"shard": to}, device_id_type=MESH)

    @pl.when(shard == 0)
    def _():
        for k in range(1, NE):
            pl.semaphore_signal(barrier, 1, device_id={"expert": other[k]}, device_id_type=MESH)

    for copy in loads(1):
        copy.start()

    def a_copy(step):
        to = row[step] + x
        return pltpu.make_async_remote_copy(
            ra.at[z], ra.at[z], a_send, a_recv, device_id={"shard": to}, device_id_type=MESH
        )

    def b_copy(step):
        to = row[0] + column[step]
        return pltpu.make_async_remote_copy(
            rb.at[x], rb.at[x], b_send, b_recv, device_id={"shard": to}, device_id_type=MESH
        )

    def c_copy(step):
        to = other[step]
        return pltpu.make_async_remote_copy(
            rb, rc.at[expert], c_send, c_recv, device_id={"expert": to}, device_id_type=MESH
        )

    def block_copy(p, dz, dx):
        to = row[dz] + column[dx]
        return pltpu.make_async_remote_copy(
            send.at[p, to],
            recv.at[p, shard],
            send_sem.at[p],
            recv_sem.at[p],
            device_id={"shard": to},
            device_id_type=MESH,
        )

    def tell(sem, step):
        for dz in (step, NZ - step):
            pl.semaphore_signal(sem, 1, device_id={"shard": row[dz] + x}, device_id_type=MESH)

    def took(ref, sem):
        pltpu.make_async_copy(ref, ref, sem).wait()

    @pl.loop(0, PAIRS)
    def _(p):
        for copy in loads(p):
            copy.wait()

        @pl.when(p + 2 < PAIRS)
        def _():
            for copy in loads(p + 2):
                copy.start()

        turned = []
        for i in range(2):
            e = 2 * p + i
            a = jnp.concatenate(
                [mg_v[e] + sg_v[e].astype(F32), mu_v[e] + su_v[e].astype(F32)], axis=0
            )
            turned.append(a.T.reshape(NS, TAKE, 128))
        send[p] = jnp.concatenate(turned, axis=1).astype(BF16)
        recv[p, shard] = send[p, shard]

        @pl.when(p == 0)
        def _():
            pl.semaphore_wait(barrier, len(NEAR) + jnp.where(shard == 0, NE - 1, 0))
            tell(near_sem, 1)

        @pl.when(p < EARLY)
        def _():
            for dz, dx in NEAR:
                block_copy(p, dz, dx).start()

        @pl.when(p == 0)
        def _():
            for copy in small:
                copy.wait()
            wide[...] = jnp.zeros((128, 128), F32)
            wide[0:16, 0:ROWS] = (rw_v[...] * rg_v[...]).astype(BF16).astype(F32)
            tall = wide[...].T
            packed = tall[0:8]
            for k in range(1, 8):
                packed = packed + pltpu.roll(tall[8 * k : 8 * k + 8], 16 * k, 1)
            ra[z] = packed.astype(BF16)

        @pl.when(p == MID)
        def _():
            pl.semaphore_wait(near_sem, 2)
            tell(mid_sem, 2)

    pl.semaphore_wait(mid_sem, 2)

    @pl.when(shard == 0)
    def _():
        for k in range(1, NE):
            pl.semaphore_signal(open_sem, 1, device_id={"expert": other[k]}, device_id_type=MESH)

    for step in range(1, NZ):
        a_copy(step).start()

    @pl.loop(0, PAIRS)
    def _(p):
        @pl.when(p < SORTED)
        def _():
            for dz, dx in FAR:
                block_copy(p, dz, dx).start()

        @pl.when((p >= EARLY) & (p < SORTED))
        def _():
            for dz, dx in NEAR:
                block_copy(p, dz, dx).start()

        @pl.when(p >= SORTED)
        def _():
            for low, high in TIERS:
                for dz in (4, 3, 5, 2, 6, 1, 7, 0):

                    @pl.when((row[dz] >= low * NX) & (row[dz] < high * NX))
                    def _():
                        for dx in (2, 1, 3, 0) if dz else (2, 1, 3):
                            block_copy(p, dz, dx).start()

        @pl.when(p == 1)
        def _():
            took(ra.at[pl.ds(0, NZ - 1)], a_recv)
            rb[x] = ra[...].astype(F32).reshape(8 * NZ, 128).astype(BF16)
            for step in range(1, NX):
                b_copy(step).start()

        @pl.when((p == 2) & (shard == 0))
        def _():
            pl.semaphore_wait(open_sem, NE - 1)
            for dz, dx in NEAR + FAR:
                to = row[dz] + column[dx]
                pl.semaphore_signal(all_sem, 1, device_id={"shard": to}, device_id_type=MESH)

        @pl.when((p == 3) & (shard != 0))
        def _():
            pl.semaphore_wait(all_sem, 1)

        @pl.when(p == 3)
        def _():
            took(rb.at[pl.ds(0, NX - 1)], b_recv)
            rc[expert] = rb[...]
            for step in range(1, NE):
                c_copy(step).start()

    def merge(p):
        took(recv.at[p, pl.ds(0, NS - 1)], recv_sem.at[p])
        merged(recv.at[p], gate.at[pl.ds(2 * p, 2)], up.at[pl.ds(2 * p, 2)])

    @pl.loop(0, PAIRS // 2)
    def _(p):
        merge(p)

    took(rc.at[pl.ds(0, NE - 1)], c_recv)
    lane = lax.broadcasted_iota(jnp.int32, (8, 128), 1) // 16

    @pl.loop(0, NX)
    def _(i):
        @pl.loop(0, NZ // 2)
        def _(h):
            total = [[None] * 8, [None] * 8]
            for e in range(NE):
                both = rc[e, i, pl.ds(pl.multiple_of(16 * h, 16), 16), :].astype(F32)
                for q in range(2):
                    one = both[8 * q : 8 * q + 8]
                    for k in range(8):
                        turn = 16 * ((e - k) % 8)
                        moved = pltpu.roll(one, turn, 1) if turn else one
                        old = total[q][k]
                        total[q][k] = moved if old is None else jnp.where(lane == e, moved, old)
            for q in range(2):
                row = pl.multiple_of(((2 * h + q) * NX + i) * ROWS, ROWS)
                router[pl.ds(row, ROWS), :] = jnp.concatenate(total[q], axis=0).astype(BF16)

    @pl.loop(PAIRS // 2, PAIRS - 1)
    def _(p):
        merge(p)

    took(recv.at[PAIRS - 1, pl.ds(0, NS - 1)], recv_sem.at[PAIRS - 1])

    @pl.loop(0, PAIRS)
    def _(p):
        took(send.at[p, pl.ds(0, NS - 1)], send_sem.at[p])

    took(ra.at[pl.ds(0, NZ - 1)], a_send)
    took(rb.at[pl.ds(0, NX - 1)], b_send)
    took(rc.at[pl.ds(0, NE - 1)], c_send)


def store(gate, up, router, recv, gate_out, up_out, router_out, gate_v, up_v, sem):
    first, last = pl.ds(0, E - 2), pl.ds(E - 2, 2)
    copies = [
        pltpu.make_async_copy(src, dst, sem.at[k])
        for k, (src, dst) in enumerate(
            (
                (gate, gate_out.at[first]),
                (up, up_out.at[first]),
                (router, router_out),
                (gate_v, gate_out.at[last]),
                (up_v, up_out.at[last]),
            )
        )
    ]
    for copy in copies[:3]:
        copy.start()
    merged(recv.at[PAIRS - 1], gate_v, up_v)
    for copy in copies[3:]:
        copy.start()
    for copy in copies:
        copy.wait()


def shards(master_gate, second_gate, master_up, second_up, router_weight, router_gain):
    dma = pltpu.SemaphoreType.DMA
    hbm, vmem = pl.BlockSpec(memory_space=pltpu.HBM), pl.BlockSpec(memory_space=pltpu.VMEM)
    shapes = (
        jax.ShapeDtypeStruct((E, TAKE, NS * ROWS), BF16),
        jax.ShapeDtypeStruct((E, TAKE, NS * ROWS), BF16),
        jax.ShapeDtypeStruct((NS * ROWS, 16 * NE), BF16),
    )
    part = jax.ShapeDtypeStruct((E - 2, TAKE, NS * ROWS), BF16)
    blocks = jax.ShapeDtypeStruct((PAIRS, NS, BLOCK, 128), BF16)
    held = pl.pallas_call(
        exchange,
        out_shape=(part, part, shapes[2], blocks),
        in_specs=[hbm] * 6,
        out_specs=(vmem,) * 4,
        scratch_shapes=[
            pltpu.VMEM((E, ROWS, COLS), F32),
            pltpu.VMEM((E, ROWS, COLS), BF16),
            pltpu.VMEM((E, ROWS, COLS), F32),
            pltpu.VMEM((E, ROWS, COLS), BF16),
            pltpu.VMEM((16, ROWS), F32),
            pltpu.VMEM((1, ROWS), F32),
            pltpu.VMEM((128, 128), F32),
            pltpu.VMEM((PAIRS, NS, BLOCK, 128), BF16),
            pltpu.VMEM((NZ, 8, 128), BF16),
            pltpu.VMEM((NX, 8 * NZ, 128), BF16),
            pltpu.VMEM((NE, NX, 8 * NZ, 128), BF16),
            dma((4, PAIRS)),
            dma((2,)),
            dma((PAIRS,)),
            dma((PAIRS,)),
        ]
        + [pltpu.SemaphoreType.REGULAR] * 4
        + [dma] * 6,
        compiler_params=pltpu.CompilerParams(
            collective_id=0, has_side_effects=True, vmem_limit_bytes=30 << 20
        ),
        name="exchange",
    )(
        *(
            pltpu.with_memory_space_constraint(a, pltpu.HBM)
            for a in (
                master_gate, second_gate, master_up, second_up,
                router_weight.T, router_gain.reshape(1, ROWS),
            )
        )
    )
    return pl.pallas_call(
        store,
        out_shape=shapes,
        in_specs=[vmem] * 4,
        out_specs=(hbm,) * 3,
        scratch_shapes=[pltpu.VMEM((2, TAKE, NS * ROWS), BF16)] * 2 + [dma((5,))],
        compiler_params=pltpu.CompilerParams(vmem_limit_bytes=8 << 20),
        name="store",
    )(*held)


def solution(mesh):
    in_specs = (P("expert", "shard", None),) * 4 + (P("shard", "expert"), P("shard"))
    out_specs = (P("expert", "shard", None), P("expert", "shard", None), P())
    return jax.shard_map(shards, mesh=mesh, in_specs=in_specs, out_specs=out_specs, check_vma=False)
```

```python
import jax
import jax.numpy as jnp
from jax import lax
from jax.experimental import pallas as pl
from jax.experimental.pallas import tpu as pltpu
from jax.sharding import PartitionSpec as P

MESH = pl.DeviceIdType.MESH
NZ, NX = 8, 4
NS = NZ * NX
NE = 8
E = 16
PAIRS = E // 2
ROWS = 64
COLS = 768
TAKE = COLS // NS
BLOCK = 2 * TAKE
F32, BF16 = jnp.float32, jnp.bfloat16
NEAR = [(dz, dx) for dz in (1, 7, 0) for dx in (2, 1, 3, 0) if dz or dx]
FAR = [(dz, dx) for dz in (4, 3, 5, 2, 6) for dx in (2, 1, 3, 0)]
EARLY = 5
SORTED = 5
TOGETHER = 6
TIERS = ((0, 2), (2, 8))
MID = 2


def merged(blocks, gate, up):
    low = lax.broadcasted_iota(jnp.int32, (BLOCK, 128), 1) < 64
    for j in range(NS // 2):
        a, b = blocks[2 * j].astype(F32), blocks[2 * j + 1].astype(F32)
        g = jnp.where(low, a, pltpu.roll(b, 64, 1))
        u = jnp.where(low, pltpu.roll(a, 64, 1), b)
        for i in range(2):
            rows = slice(TAKE * i, TAKE * (i + 1))
            gate[i, :, 128 * j : 128 * (j + 1)] = g[rows].astype(BF16)
            up[i, :, 128 * j : 128 * (j + 1)] = u[rows].astype(BF16)


def exchange(
    mg, sg, mu, su, rw, rg,
    gate, up, router, recv,
    mg_v, sg_v, mu_v, su_v, rw_v, rg_v, wide, send, ra, rb, rc,
    load_sem, small_sem, send_sem, recv_sem, near_sem, mid_sem, open_sem, all_sem, a_send, a_recv, b_send, b_recv, c_send, c_recv,
):
    shard, expert = lax.axis_index("shard"), lax.axis_index("expert")
    z, x = shard // NX, shard % NX
    row = [lax.rem(z + k, NZ) * NX for k in range(NZ)]
    column = [lax.rem(x + k, NX) for k in range(NX)]
    other = [lax.rem(expert + k, NE) for k in range(NE)]

    def loads(p):
        at = pl.ds(2 * p, 2)
        return [
            pltpu.make_async_copy(src.at[at], dst.at[at], load_sem.at[k, p])
            for k, (src, dst) in enumerate(((mg, mg_v), (sg, sg_v), (mu, mu_v), (su, su_v)))
        ]

    for copy in loads(0):
        copy.start()
    small = (
        pltpu.make_async_copy(rw, rw_v, small_sem.at[0]),
        pltpu.make_async_copy(rg, rg_v, small_sem.at[1]),
    )
    for copy in small:
        copy.start()

    barrier = pltpu.get_barrier_semaphore()

    for dz, dx in NEAR:
        to = row[dz] + column[dx]
        pl.semaphore_signal(barrier, 1, device_id={"shard": to}, device_id_type=MESH)

    @pl.when(shard == 0)
    def _():
        for k in range(1, NE):
            pl.semaphore_signal(barrier, 1, device_id={"expert": other[k]}, device_id_type=MESH)

    for copy in loads(1):
        copy.start()

    def a_copy(step):
        to = row[step] + x
        return pltpu.make_async_remote_copy(
            ra.at[z], ra.at[z], a_send, a_recv, device_id={"shard": to}, device_id_type=MESH
        )

    def b_copy(step):
        to = row[0] + column[step]
        return pltpu.make_async_remote_copy(
            rb.at[x], rb.at[x], b_send, b_recv, device_id={"shard": to}, device_id_type=MESH
        )

    def c_copy(step):
        to = other[step]
        return pltpu.make_async_remote_copy(
            rb, rc.at[expert], c_send, c_recv, device_id={"expert": to}, device_id_type=MESH
        )

    def block_copy(p, dz, dx):
        to = row[dz] + column[dx]
        return pltpu.make_async_remote_copy(
            send.at[p, to],
            recv.at[p, shard],
            send_sem.at[p],
            recv_sem.at[p],
            device_id={"shard": to},
            device_id_type=MESH,
        )

    def tell(sem, step):
        for dz in (step, NZ - step):
            pl.semaphore_signal(sem, 1, device_id={"shard": row[dz] + x}, device_id_type=MESH)

    def took(ref, sem):
        pltpu.make_async_copy(ref, ref, sem).wait()

    @pl.loop(0, PAIRS)
    def _(p):
        for copy in loads(p):
            copy.wait()

        @pl.when(p + 2 < PAIRS)
        def _():
            for copy in loads(p + 2):
                copy.start()

        turned = []
        for i in range(2):
            e = 2 * p + i
            a = jnp.concatenate(
                [mg_v[e] + sg_v[e].astype(F32), mu_v[e] + su_v[e].astype(F32)], axis=0
            )
            turned.append(a.T.reshape(NS, TAKE, 128))
        send[p] = jnp.concatenate(turned, axis=1).astype(BF16)
        recv[p, shard] = send[p, shard]

        @pl.when(p == 0)
        def _():
            pl.semaphore_wait(barrier, len(NEAR) + jnp.where(shard == 0, NE - 1, 0))
            tell(near_sem, 1)

        @pl.when(p < EARLY)
        def _():
            for dz, dx in NEAR:
                block_copy(p, dz, dx).start()

        @pl.when(p == 0)
        def _():
            for copy in small:
                copy.wait()
            wide[...] = jnp.zeros((128, 128), F32)
            wide[0:16, 0:ROWS] = (rw_v[...] * rg_v[...]).astype(BF16).astype(F32)
            tall = wide[...].T
            packed = tall[0:8]
            for k in range(1, 8):
                packed = packed + pltpu.roll(tall[8 * k : 8 * k + 8], 16 * k, 1)
            ra[z] = packed.astype(BF16)

        @pl.when(p == MID)
        def _():
            pl.semaphore_wait(near_sem, 2)
            tell(mid_sem, 2)

    pl.semaphore_wait(mid_sem, 2)

    @pl.when(shard == 0)
    def _():
        for k in range(1, NE):
            pl.semaphore_signal(open_sem, 1, device_id={"expert": other[k]}, device_id_type=MESH)

    for step in range(1, NZ):
        a_copy(step).start()

    @pl.loop(0, PAIRS)
    def _(p):
        @pl.when(p < SORTED)
        def _():
            for dz, dx in FAR:
                block_copy(p, dz, dx).start()

        @pl.when((p >= EARLY) & (p < SORTED))
        def _():
            for dz, dx in NEAR:
                block_copy(p, dz, dx).start()

        def send_tier(p, low, high):
            for dz in (4, 3, 5, 2, 6, 1, 7, 0):

                @pl.when((row[dz] >= low * NX) & (row[dz] < high * NX))
                def _():
                    for dx in (2, 1, 3, 0) if dz else (2, 1, 3):
                        block_copy(p, dz, dx).start()

        @pl.when((p >= SORTED) & (p < TOGETHER))
        def _():
            for low, high in TIERS:
                send_tier(p, low, high)

        @pl.when(p == TOGETHER)
        def _():
            for low, high in TIERS:

                @pl.loop(TOGETHER, PAIRS)
                def _(q):
                    send_tier(q, low, high)

        @pl.when(p == 1)
        def _():
            took(ra.at[pl.ds(0, NZ - 1)], a_recv)
            rb[x] = ra[...].astype(F32).reshape(8 * NZ, 128).astype(BF16)
            for step in range(1, NX):
                b_copy(step).start()

        @pl.when((p == 2) & (shard == 0))
        def _():
            pl.semaphore_wait(open_sem, NE - 1)
            for dz, dx in NEAR + FAR:
                to = row[dz] + column[dx]
                pl.semaphore_signal(all_sem, 1, device_id={"shard": to}, device_id_type=MESH)

        @pl.when((p == 3) & (shard != 0))
        def _():
            pl.semaphore_wait(all_sem, 1)

        @pl.when(p == 3)
        def _():
            took(rb.at[pl.ds(0, NX - 1)], b_recv)
            rc[expert] = rb[...]
            for step in range(1, NE):
                c_copy(step).start()

    def merge(p):
        took(recv.at[p, pl.ds(0, NS - 1)], recv_sem.at[p])
        merged(recv.at[p], gate.at[pl.ds(2 * p, 2)], up.at[pl.ds(2 * p, 2)])

    @pl.loop(0, PAIRS // 2)
    def _(p):
        merge(p)

    took(rc.at[pl.ds(0, NE - 1)], c_recv)
    lane = lax.broadcasted_iota(jnp.int32, (8, 128), 1) // 16

    @pl.loop(0, NX)
    def _(i):
        @pl.loop(0, NZ // 2)
        def _(h):
            total = [[None] * 8, [None] * 8]
            for e in range(NE):
                both = rc[e, i, pl.ds(pl.multiple_of(16 * h, 16), 16), :].astype(F32)
                for q in range(2):
                    one = both[8 * q : 8 * q + 8]
                    for k in range(8):
                        turn = 16 * ((e - k) % 8)
                        moved = pltpu.roll(one, turn, 1) if turn else one
                        old = total[q][k]
                        total[q][k] = moved if old is None else jnp.where(lane == e, moved, old)
            for q in range(2):
                row = pl.multiple_of(((2 * h + q) * NX + i) * ROWS, ROWS)
                router[pl.ds(row, ROWS), :] = jnp.concatenate(total[q], axis=0).astype(BF16)

    @pl.loop(PAIRS // 2, PAIRS - 1)
    def _(p):
        merge(p)

    took(recv.at[PAIRS - 1, pl.ds(0, NS - 1)], recv_sem.at[PAIRS - 1])

    @pl.loop(0, PAIRS)
    def _(p):
        took(send.at[p, pl.ds(0, NS - 1)], send_sem.at[p])

    took(ra.at[pl.ds(0, NZ - 1)], a_send)
    took(rb.at[pl.ds(0, NX - 1)], b_send)
    took(rc.at[pl.ds(0, NE - 1)], c_send)


def store(gate, up, router, recv, gate_out, up_out, router_out, gate_v, up_v, sem):
    first, last = pl.ds(0, E - 2), pl.ds(E - 2, 2)
    copies = [
        pltpu.make_async_copy(src, dst, sem.at[k])
        for k, (src, dst) in enumerate(
            (
                (gate, gate_out.at[first]),
                (up, up_out.at[first]),
                (router, router_out),
                (gate_v, gate_out.at[last]),
                (up_v, up_out.at[last]),
            )
        )
    ]
    for copy in copies[:3]:
        copy.start()
    merged(recv.at[PAIRS - 1], gate_v, up_v)
    for copy in copies[3:]:
        copy.start()
    for copy in copies:
        copy.wait()


def shards(master_gate, second_gate, master_up, second_up, router_weight, router_gain):
    dma = pltpu.SemaphoreType.DMA
    hbm, vmem = pl.BlockSpec(memory_space=pltpu.HBM), pl.BlockSpec(memory_space=pltpu.VMEM)
    shapes = (
        jax.ShapeDtypeStruct((E, TAKE, NS * ROWS), BF16),
        jax.ShapeDtypeStruct((E, TAKE, NS * ROWS), BF16),
        jax.ShapeDtypeStruct((NS * ROWS, 16 * NE), BF16),
    )
    part = jax.ShapeDtypeStruct((E - 2, TAKE, NS * ROWS), BF16)
    blocks = jax.ShapeDtypeStruct((PAIRS, NS, BLOCK, 128), BF16)
    held = pl.pallas_call(
        exchange,
        out_shape=(part, part, shapes[2], blocks),
        in_specs=[hbm] * 6,
        out_specs=(vmem,) * 4,
        scratch_shapes=[
            pltpu.VMEM((E, ROWS, COLS), F32),
            pltpu.VMEM((E, ROWS, COLS), BF16),
            pltpu.VMEM((E, ROWS, COLS), F32),
            pltpu.VMEM((E, ROWS, COLS), BF16),
            pltpu.VMEM((16, ROWS), F32),
            pltpu.VMEM((1, ROWS), F32),
            pltpu.VMEM((128, 128), F32),
            pltpu.VMEM((PAIRS, NS, BLOCK, 128), BF16),
            pltpu.VMEM((NZ, 8, 128), BF16),
            pltpu.VMEM((NX, 8 * NZ, 128), BF16),
            pltpu.VMEM((NE, NX, 8 * NZ, 128), BF16),
            dma((4, PAIRS)),
            dma((2,)),
            dma((PAIRS,)),
            dma((PAIRS,)),
        ]
        + [pltpu.SemaphoreType.REGULAR] * 4
        + [dma] * 6,
        compiler_params=pltpu.CompilerParams(
            collective_id=0, has_side_effects=True, vmem_limit_bytes=30 << 20
        ),
        name="exchange",
    )(
        *(
            pltpu.with_memory_space_constraint(a, pltpu.HBM)
            for a in (
                master_gate, second_gate, master_up, second_up,
                router_weight.T, router_gain.reshape(1, ROWS),
            )
        )
    )
    return pl.pallas_call(
        store,
        out_shape=shapes,
        in_specs=[vmem] * 4,
        out_specs=(hbm,) * 3,
        scratch_shapes=[pltpu.VMEM((2, TAKE, NS * ROWS), BF16)] * 2 + [dma((5,))],
        compiler_params=pltpu.CompilerParams(vmem_limit_bytes=8 << 20),
        name="store",
    )(*held)


def solution(mesh):
    in_specs = (P("expert", "shard", None),) * 4 + (P("shard", "expert"), P("shard"))
    out_specs = (P("expert", "shard", None), P("expert", "shard", None), P())
    return jax.shard_map(shards, mesh=mesh, in_specs=in_specs, out_specs=out_specs, check_vma=False)
```
